32 devices in a mesh: ang: 16 (over z, y, core), sl: 2 (over x).
Axes of the slice: x: 2, y: 2, z: 4, core: 2. Of those that a mesh axis runs over, the one named last changes fastest.
Arguments:
- sinogram: bfloat16 [16, 32, 1024], P('sl', 'ang'), may hold values from -72 to 72
- detector_coord: int32 [32, 32, 512], P('ang', 'sl'), may hold values from 0 to 1072693247
Outputs:
- image_rows: float32 [32, 16, 512], P('ang', 'sl')
The draws below stay inside these ranges and needn't reach their ends.
All inputs are finite; a program needn't handle non-finite values.
Results may differ from the reference program's by a relative error of at most 0.0052.
Values may be sent and summed in bfloat16 or wider, within the bound.
A program may use at most 64 MiB of HBM per device.

```python
import math
import jax
import jax.numpy as jnp
from jax import lax

BINS = 1024
IMG = 512
SLICES = 16
ANGLES = 32
ROWS = 32


def place_ends(result, own_key, least, high):
    index_at = [jax.random.randint(jax.random.fold_in(own_key, axis), (), 0, length) for axis, length in enumerate(result.shape)]
    longest = result.shape.index(max(result.shape))
    beside = index_at[:longest] + [(index_at[longest] + 1) % result.shape[longest]] + index_at[longest + 1:]
    return result.at[tuple(index_at)].set(least).at[tuple(beside)].set(high)


def levels(key, shape, split, low, high):
    gain, own = 1.0, jax.random.fold_in(key, 6)
    for dim, parts in split:
        heights = jnp.exp(jax.random.uniform(jax.random.fold_in(own, dim), (parts,), jnp.float32, low / len(split), high / len(split)))
        gain = gain * jnp.repeat(heights, shape[dim] // parts).reshape([-1 if axis == dim else 1 for axis in range(len(shape))])
    return gain


def bell_draw(rng, dims, scale, reach, shards=(), kind=jnp.bfloat16):
    values = scale * jax.random.normal(rng, dims, jnp.float32)
    if shards:
        values = values * levels(rng, dims, shards, -0.22, 0.18)
    return jnp.clip(values, -reach, reach).astype(kind)


def setup_inputs(seed: int = 0) -> dict:
    key_list = jax.random.split(jax.random.key(seed), 3)
    return {
        "sinogram": bell_draw(key_list[0], (SLICES, ANGLES, BINS), 12.0, 72.0, ((0, 2), (1, 16))),
        "detector_coord": place_ends(jax.random.randint(key_list[1], (ANGLES, ROWS, IMG), 0, (BINS - 1) * 1048576), jax.random.fold_in(key_list[1], 1), 0, ((BINS - 1) * 1048576) - 1).astype(jnp.int32),
    }


def ramp_table(bin_count):
    first = lax.broadcasted_iota(jnp.int32, (bin_count, bin_count), 0)
    second = lax.broadcasted_iota(jnp.int32, (bin_count, bin_count), 1)
    offset = second - first
    offset_sq = jnp.maximum((offset * offset).astype(jnp.float32), jnp.float32(1.0))
    odd_mask = (offset % 2) != 0
    values = jnp.where(offset == 0, jnp.float32(0.25), jnp.where(odd_mask, jnp.float32(-1.0 / (math.pi ** 2)) / offset_sq, jnp.float32(0.0)))
    return values.astype(jnp.bfloat16)


def interp_weights(row_coords, bin_count):
    bin_left = row_coords // 1048576
    fraction = (row_coords % 1048576).astype(jnp.float32) / jnp.float32(1048576.0)
    positions = lax.broadcasted_iota(jnp.int32, row_coords.shape + (bin_count,), 2)
    left_part = jnp.where(positions == bin_left[..., None], 1.0 - fraction[..., None], jnp.float32(0.0))
    right_part = jnp.where(positions == bin_left[..., None] + 1, fraction[..., None], jnp.float32(0.0))
    return (left_part + right_part).astype(jnp.bfloat16)


def reference(sinogram, detector_coord):
    slices, angles, bin_count = sinogram.shape
    table = ramp_table(bin_count)
    filtered = jnp.dot(sinogram.reshape(slices * angles, bin_count), table, preferred_element_type=jnp.float32)
    filtered = filtered.astype(jnp.bfloat16).reshape(slices, angles, bin_count)

    def add_angle(running, angle_step):
        projection = lax.dynamic_index_in_dim(filtered, angle_step, 1, keepdims=False)
        row_coords = lax.dynamic_index_in_dim(detector_coord, angle_step, 0, keepdims=False)
        weights = interp_weights(row_coords, bin_count)
        contrib = jnp.einsum('rxb,sb->rsx', weights.astype(jnp.float32), projection.astype(jnp.float32))
        return running + contrib, None

    start_value = jnp.zeros((detector_coord.shape[1], slices, detector_coord.shape[2]), jnp.float32)
    running, unused = lax.scan(add_angle, start_value, jnp.arange(angles, dtype=jnp.int32))
    return running * jnp.float32(math.pi / angles)
```

```python
import functools
import math

import jax
import jax.numpy as jnp
from jax import lax
from jax.experimental import pallas as pl
from jax.experimental.pallas import tpu as pltpu
from jax.sharding import PartitionSpec as P

LANES = 128
FRACTION_BITS = 20


def ramp_block(size, shift):
    first = lax.broadcasted_iota(jnp.int32, (size, size), 0)
    second = lax.broadcasted_iota(jnp.int32, (size, size), 1)
    offset = second - first + shift
    offset_sq = jnp.maximum((offset * offset).astype(jnp.float32), jnp.float32(1.0))
    values = jnp.where(
        offset == 0,
        jnp.float32(0.25),
        jnp.where(
            (offset & 1) != 0, jnp.float32(-1.0 / math.pi**2) / offset_sq, jnp.float32(0.0)
        ),
    )
    return values.astype(jnp.bfloat16)


def build_ramp(ramp, size, count):
    for step in range(2 * count - 1):
        ramp[step] = ramp_block(size, (step - count + 1) * size)


def filter_rows(sino, ramp, tiles, size, count):
    rows = sino.shape[0]
    per_row = sino.shape[1] // LANES
    for out_block in range(count):
        total = None
        for in_block in range(count):
            part = jnp.dot(
                sino[:, in_block * size : (in_block + 1) * size],
                ramp[out_block - in_block + count - 1],
                preferred_element_type=jnp.float32,
            )
            total = part if total is None else total + part
        total = total.astype(jnp.bfloat16).astype(jnp.float32)
        for piece in range(size // LANES):
            h = out_block * (size // LANES) + piece
            tiles[pl.ds(h, rows, stride=per_row), :] = total[:, piece * LANES : (piece + 1) * LANES]


def pick(tile, index):
    return jnp.take_along_axis(tile, index, axis=1, mode="promise_in_bounds")


def interpolate(coords, tiles, out, scale, angles, slices, per_row, together=2):
    rows, width = coords.shape[-2], coords.shape[-1]
    level = lax.broadcasted_iota(jnp.int32, (per_row, LANES), 0)
    spots = [(r, x) for r in range(rows) for x in range(width // LANES)]
    for start in range(0, len(spots), together):
        group = spots[start : start + together]

        def one_angle(a, sums):
            picks = []
            for r, x in group:
                c = coords[a, pl.ds(r, 1), pl.ds(x * LANES, LANES)]
                c = jnp.broadcast_to(c, (per_row, LANES))
                left = c >> FRACTION_BITS
                right = left + 1
                fraction = (c & (2**FRACTION_BITS - 1)).astype(jnp.float32) * jnp.float32(
                    2.0**-FRACTION_BITS
                )
                w_left = (1.0 - fraction).astype(jnp.bfloat16).astype(jnp.float32)
                w_right = fraction.astype(jnp.bfloat16).astype(jnp.float32)
                w_left = jnp.where(left >> 7 == level, w_left, 0.0)
                w_right = jnp.where(right >> 7 == level, w_right, 0.0)
                picks.append((left & (LANES - 1), right & (LANES - 1), w_left, w_right))
            new = []
            for s in range(slices):
                row = pl.multiple_of((s * angles + a) * per_row, per_row)
                tile = tiles[pl.ds(row, per_row), :]
                for g, (i_left, i_right, w_left, w_right) in enumerate(picks):
                    term = w_left * pick(tile, i_left) + w_right * pick(tile, i_right)
                    new.append(sums[s * len(group) + g] + term)
            return tuple(new)

        zero = jnp.zeros((per_row, LANES), jnp.float32)
        sums = lax.fori_loop(0, angles, one_angle, (zero,) * (slices * len(group)), unroll=2)
        for s in range(slices):
            for g, (r, x) in enumerate(group):
                line = jnp.sum(sums[s * len(group) + g], axis=0, keepdims=True) * scale
                out[r, pl.ds(s, 1), pl.ds(x * LANES, LANES)] = line


def kernel(angles, slices, sino, coords, out, ramp, tiles):
    bins = sino.shape[1]
    size = ramp.shape[1]
    build_ramp(ramp, size, bins // size)
    filter_rows(sino, ramp, tiles, size, bins // size)
    scale = jnp.float32(math.pi / angles)
    interpolate(coords, tiles, out, scale, angles, slices, bins // LANES)


def shards(sinogram, detector_coord):
    slices, own_angles, bins = sinogram.shape
    width = detector_coord.shape[2]
    groups = lax.axis_size("ang")
    angles = own_angles * groups
    coord_table = lax.all_gather(detector_coord, "sl", axis=1, tiled=True)
    row_share = coord_table.shape[1] // groups
    own_rows = lax.all_to_all(coord_table, "ang", split_axis=1, concat_axis=0, tiled=True)
    sino = lax.all_gather(sinogram, "ang", axis=1, tiled=True).reshape(slices * angles, bins)
    size = 256
    return pl.pallas_call(
        functools.partial(kernel, angles, slices),
        out_shape=jax.ShapeDtypeStruct((row_share, slices, width), jnp.float32),
        in_specs=[pl.BlockSpec(memory_space=pltpu.VMEM)] * 2,
        out_specs=pl.BlockSpec(memory_space=pltpu.VMEM),
        scratch_shapes=[
            pltpu.VMEM((2 * (bins // size) - 1, size, size), jnp.bfloat16),
            pltpu.VMEM((slices * angles * bins // LANES, LANES), jnp.float32),
        ],
    )(sino, own_rows)


def solution(mesh):
    in_specs = (P("sl", "ang", None), P("ang", "sl", None))
    out_specs = P("ang", "sl", None)
    return jax.shard_map(shards, mesh=mesh, in_specs=in_specs, out_specs=out_specs, check_vma=False)
```

```python
import functools
import math

import jax
import jax.numpy as jnp
from jax import lax
from jax.experimental import pallas as pl
from jax.experimental.pallas import tpu as pltpu
from jax.sharding import PartitionSpec as P

LANES = 128
FRACTION_BITS = 20


def ramp_block(size, shift):
    first = lax.broadcasted_iota(jnp.int32, (size, size), 0)
    second = lax.broadcasted_iota(jnp.int32, (size, size), 1)
    offset = second - first + shift
    offset_sq = jnp.maximum((offset * offset).astype(jnp.float32), jnp.float32(1.0))
    values = jnp.where(
        offset == 0,
        jnp.float32(0.25),
        jnp.where(
            (offset & 1) != 0, jnp.float32(-1.0 / math.pi**2) / offset_sq, jnp.float32(0.0)
        ),
    )
    return values.astype(jnp.bfloat16)


def build_ramp(ramp, size, count):
    for step in range(2 * count - 1):
        ramp[step] = ramp_block(size, (step - count + 1) * size)


def filter_rows(sino, ramp, tiles, size, count):
    rows = sino.shape[0]
    per_row = sino.shape[1] // LANES
    for out_block in range(count):
        total = None
        for in_block in range(count):
            part = jnp.dot(
                sino[:, in_block * size : (in_block + 1) * size],
                ramp[out_block - in_block + count - 1],
                preferred_element_type=jnp.float32,
            )
            total = part if total is None else total + part
        total = total.astype(jnp.bfloat16).astype(jnp.float32)
        for piece in range(size // LANES):
            h = out_block * (size // LANES) + piece
            tiles[pl.ds(h, rows, stride=per_row), :] = total[:, piece * LANES : (piece + 1) * LANES]


def pick(tile, index):
    return jnp.take_along_axis(tile, index, axis=1, mode="promise_in_bounds")


def interpolate(coords, tiles, out, scale, own_angles, together=2):
    rows, slices, width = out.shape
    groups = coords.shape[0]
    per_row = tiles.shape[0] // (groups * slices * own_angles)
    across = width // LANES
    level = lax.broadcasted_iota(jnp.int32, (per_row, LANES), 0)
    spots = [(r, x) for r in range(rows) for x in range(across)]
    for start in range(0, len(spots), together):
        group = spots[start : start + together]

        def one_group(g, sums):
            sums = list(sums)
            for al in range(own_angles):
                picks = []
                for r, x in group:
                    c = coords[g, pl.ds((al * rows + r) * across + x, 1), :]
                    c = jnp.broadcast_to(c, (per_row, LANES))
                    left = c >> FRACTION_BITS
                    right = left + 1
                    fraction = (c & (2**FRACTION_BITS - 1)).astype(jnp.float32) * jnp.float32(
                        2.0**-FRACTION_BITS
                    )
                    w_left = (1.0 - fraction).astype(jnp.bfloat16).astype(jnp.float32)
                    w_right = fraction.astype(jnp.bfloat16).astype(jnp.float32)
                    w_left = jnp.where(left >> 7 == level, w_left, 0.0)
                    w_right = jnp.where(right >> 7 == level, w_right, 0.0)
                    picks.append((left & (LANES - 1), right & (LANES - 1), w_left, w_right))
                for s in range(slices):
                    row = ((g * slices + s) * own_angles + al) * per_row
                    tile = tiles[pl.ds(pl.multiple_of(row, per_row), per_row), :]
                    for i, (i_left, i_right, w_left, w_right) in enumerate(picks):
                        term = w_left * pick(tile, i_left) + w_right * pick(tile, i_right)
                        sums[s * len(group) + i] = sums[s * len(group) + i] + term
            return tuple(sums)

        zero = jnp.zeros((per_row, LANES), jnp.float32)
        sums = lax.fori_loop(0, groups, one_group, (zero,) * (slices * len(group)))
        for s in range(slices):
            for i, (r, x) in enumerate(group):
                line = jnp.sum(sums[s * len(group) + i], axis=0, keepdims=True) * scale
                out[r, pl.ds(s, 1), pl.ds(x * LANES, LANES)] = line


def project_kernel(own_angles, sino, coords, out, ramp, tiles):
    bins = sino.shape[1]
    size = ramp.shape[1]
    build_ramp(ramp, size, bins // size)
    filter_rows(sino, ramp, tiles, size, bins // size)
    scale = jnp.float32(math.pi / (own_angles * coords.shape[0]))
    interpolate(coords, tiles, out, scale, own_angles)


def exchange_kernel(
    groups, halves, sino, coords, all_sino, all_coords,
    local_sem, s_send, s_recv, f_send, c_send, c_recv,
):
    me, half = lax.axis_index("ang"), lax.axis_index("sl")
    chip, core = me // 2, me % 2
    chips = groups // 2
    mate = chip * 2 + 1 - core
    total = groups * halves
    share = coords.shape[0]

    barrier = pltpu.get_barrier_semaphore()

    def greet(k, carry):
        there = lax.rem(me * halves + half + k, total)
        pl.semaphore_signal(
            barrier, inc=1, device_id={"ang": there // halves, "sl": there % halves},
            device_id_type=pl.DeviceIdType.MESH,
        )
        return carry

    lax.fori_loop(1, total, greet, 0)
    own = pltpu.make_async_copy(sino, all_sino.at[me], local_sem.at[0])
    own.start()
    pl.semaphore_wait(barrier, total - 1)

    def sino_copy(source, block, target, send_sem):
        return pltpu.make_async_remote_copy(
            src_ref=source, dst_ref=all_sino.at[block], send_sem=send_sem,
            recv_sem=s_recv.at[block], device_id={"ang": target},
            device_id_type=pl.DeviceIdType.MESH,
        )

    for k in range(chips - 1, 0, -1):
        sino_copy(sino, me, lax.rem(chip + k, chips) * 2 + core, s_send.at[k]).start()
    sino_copy(sino, me, mate, f_send.at[0]).start()

    def coord_copy(j, t):
        place = lax.rem(me + j, share)
        side = lax.rem(half + t, halves)
        target = half * share + place
        return target, side, coords.at[place], c_send.at[j * halves + t]

    def coord_remote(j, t):
        target, side, block, sem = coord_copy(j, t)
        return pltpu.make_async_remote_copy(
            src_ref=block, dst_ref=all_coords.at[me], send_sem=sem,
            recv_sem=c_recv.at[me], device_id={"ang": target, "sl": side},
            device_id_type=pl.DeviceIdType.MESH,
        )

    source_half = me // share
    at_home = source_half == half
    for j in range(share):
        for t in range(halves):
            if j == 0 and t == 0:
                @pl.when(at_home)
                def _():
                    pltpu.make_async_copy(
                        coords.at[lax.rem(me, share)], all_coords.at[me], c_recv.at[me]
                    ).start()

                @pl.when(jnp.logical_not(at_home))
                def _():
                    coord_remote(0, 0).start()
            else:
                coord_remote(j, t).start()

    for k in range(1, chips):
        block = lax.rem(chip + k, chips) * 2 + core
        sino_copy(sino, block, mate, f_send.at[k]).wait_recv()
        sino_copy(all_sino.at[block], block, mate, f_send.at[k]).start()
    for k in range(chips):
        block = lax.rem(chip + k, chips) * 2 + 1 - core
        sino_copy(sino, block, mate, f_send.at[0]).wait_recv()
    for g in range(groups):
        pltpu.make_async_copy(coords.at[0], all_coords.at[g], c_recv.at[g]).wait()
    own.wait()
    for k in range(1, chips):
        sino_copy(sino, me, mate, s_send.at[k]).wait_send()
    for k in range(chips):
        sino_copy(sino, me, mate, f_send.at[k]).wait_send()
    for j in range(share):
        for t in range(halves):
            if j == 0 and t == 0:
                @pl.when(jnp.logical_not(at_home))
                def _():
                    coord_remote(0, 0).wait_send()
            else:
                coord_remote(j, t).wait_send()


def shards(sinogram, detector_coord):
    slices, own_angles, bins = sinogram.shape
    local_rows, width = detector_coord.shape[1:]
    groups, halves = lax.axis_size("ang"), lax.axis_size("sl")
    row_share = local_rows * halves // groups
    share = local_rows // row_share
    sino = sinogram.reshape(slices * own_angles, bins)
    coords = detector_coord.reshape(own_angles, share, row_share, width)
    coords = coords.transpose(1, 0, 2, 3).reshape(share, -1, LANES)
    vmem = pl.BlockSpec(memory_space=pltpu.VMEM)
    all_sino, all_coords = pl.pallas_call(
        functools.partial(exchange_kernel, groups, halves),
        out_shape=(
            jax.ShapeDtypeStruct((groups,) + sino.shape, sino.dtype),
            jax.ShapeDtypeStruct((groups,) + coords.shape[1:], coords.dtype),
        ),
        in_specs=[vmem] * 2,
        out_specs=(vmem, vmem),
        scratch_shapes=[
            pltpu.SemaphoreType.DMA((1,)),
            pltpu.SemaphoreType.DMA((groups // 2,)),
            pltpu.SemaphoreType.DMA((groups,)),
            pltpu.SemaphoreType.DMA((groups // 2,)),
            pltpu.SemaphoreType.DMA((groups,)),
            pltpu.SemaphoreType.DMA((groups,)),
        ],
        compiler_params=pltpu.CompilerParams(collective_id=0, has_side_effects=True),
    )(sino, coords)
    size = 256
    return pl.pallas_call(
        functools.partial(project_kernel, own_angles),
        out_shape=jax.ShapeDtypeStruct((row_share, slices, width), jnp.float32),
        in_specs=[vmem] * 2,
        out_specs=vmem,
        scratch_shapes=[
            pltpu.VMEM((2 * (bins // size) - 1, size, size), jnp.bfloat16),
            pltpu.VMEM((groups * slices * own_angles * bins // LANES, LANES), jnp.float32),
        ],
    )(all_sino.reshape(groups * slices * own_angles, bins), all_coords)


def solution(mesh):
    in_specs = (P("sl", "ang", None), P("ang", "sl", None))
    out_specs = P("ang", "sl", None)
    return jax.shard_map(shards, mesh=mesh, in_specs=in_specs, out_specs=out_specs, check_vma=False)
```

```python
import functools
import math

import jax
import jax.numpy as jnp
from jax import lax
from jax.experimental import pallas as pl
from jax.experimental.pallas import tpu as pltpu
from jax.sharding import PartitionSpec as P

LANES = 128
FRACTION_BITS = 20


def ramp_block(size, shift):
    first = lax.broadcasted_iota(jnp.int32, (size, size), 0)
    second = lax.broadcasted_iota(jnp.int32, (size, size), 1)
    offset = second - first + shift
    offset_sq = jnp.maximum((offset * offset).astype(jnp.float32), jnp.float32(1.0))
    values = jnp.where(
        offset == 0,
        jnp.float32(0.25),
        jnp.where(
            (offset & 1) != 0, jnp.float32(-1.0 / math.pi**2) / offset_sq, jnp.float32(0.0)
        ),
    )
    return values.astype(jnp.bfloat16)


def build_ramp(ramp, size, count):
    for step in range(2 * count - 1):
        ramp[step] = ramp_block(size, (step - count + 1) * size)


def filter_rows(sino, ramp, tiles, size, count):
    rows = sino.shape[0]
    per_row = sino.shape[1] // LANES
    for out_block in range(count):
        total = None
        for in_block in range(count):
            part = jnp.dot(
                sino[:, in_block * size : (in_block + 1) * size],
                ramp[out_block - in_block + count - 1],
                preferred_element_type=jnp.float32,
            )
            total = part if total is None else total + part
        total = total.astype(jnp.bfloat16).astype(jnp.float32)
        for piece in range(size // LANES):
            h = out_block * (size // LANES) + piece
            tiles[pl.ds(h, rows, stride=per_row), :] = total[:, piece * LANES : (piece + 1) * LANES]


def pick(tile, index):
    return jnp.take_along_axis(tile, index, axis=1, mode="promise_in_bounds")


def interpolate(coords, tiles, out, scale, own_angles, together=2):
    rows, slices, width = out.shape
    groups = coords.shape[0]
    per_row = tiles.shape[0] // (groups * slices * own_angles)
    across = width // LANES
    level = lax.broadcasted_iota(jnp.int32, (per_row, LANES), 0)
    spots = [(r, x) for r in range(rows) for x in range(across)]
    for start in range(0, len(spots), together):
        group = spots[start : start + together]

        def one_group(g, sums):
            sums = list(sums)
            for al in range(own_angles):
                picks = []
                for r, x in group:
                    c = coords[g, pl.ds((al * rows + r) * across + x, 1), :]
                    c = jnp.broadcast_to(c, (per_row, LANES))
                    left = c >> FRACTION_BITS
                    right = left + 1
                    fraction = (c & (2**FRACTION_BITS - 1)).astype(jnp.float32) * jnp.float32(
                        2.0**-FRACTION_BITS
                    )
                    w_left = (1.0 - fraction).astype(jnp.bfloat16).astype(jnp.float32)
                    w_right = fraction.astype(jnp.bfloat16).astype(jnp.float32)
                    w_left = jnp.where(left >> 7 == level, w_left, 0.0)
                    w_right = jnp.where(right >> 7 == level, w_right, 0.0)
                    picks.append((left & (LANES - 1), right & (LANES - 1), w_left, w_right))
                held = []
                for s in range(slices):
                    row = ((g * slices + s) * own_angles + al) * per_row
                    held.append(tiles[pl.ds(pl.multiple_of(row, per_row), per_row), :])
                for i, (i_left, i_right, w_left, w_right) in enumerate(picks):
                    for index, weight in ((i_left, w_left), (i_right, w_right)):
                        for s in range(slices):
                            at = s * len(group) + i
                            sums[at] = sums[at] + weight * pick(held[s], index)
            return tuple(sums)

        zero = jnp.zeros((per_row, LANES), jnp.float32)
        sums = lax.fori_loop(0, groups, one_group, (zero,) * (slices * len(group)))
        for s in range(slices):
            for i, (r, x) in enumerate(group):
                line = jnp.sum(sums[s * len(group) + i], axis=0, keepdims=True) * scale
                out[r, pl.ds(s, 1), pl.ds(x * LANES, LANES)] = line


def project_kernel(own_angles, sino, coords, out, ramp, tiles):
    bins = sino.shape[1]
    size = ramp.shape[1]
    build_ramp(ramp, size, bins // size)
    filter_rows(sino, ramp, tiles, size, bins // size)
    scale = jnp.float32(math.pi / (own_angles * coords.shape[0]))
    interpolate(coords, tiles, out, scale, own_angles)


def exchange_kernel(
    groups, halves, sino, coords, all_sino, all_coords,
    local_sem, s_send, s_recv, f_send, c_send, c_recv,
):
    me, half = lax.axis_index("ang"), lax.axis_index("sl")
    chip, core = me // 2, me % 2
    chips = groups // 2
    mate = chip * 2 + 1 - core
    total = groups * halves
    share = coords.shape[0]

    barrier = pltpu.get_barrier_semaphore()

    def greet(k, carry):
        there = lax.rem(me * halves + half + k, total)
        pl.semaphore_signal(
            barrier, inc=1, device_id={"ang": there // halves, "sl": there % halves},
            device_id_type=pl.DeviceIdType.MESH,
        )
        return carry

    lax.fori_loop(1, total, greet, 0)
    own = pltpu.make_async_copy(sino, all_sino.at[me], local_sem.at[0])
    own.start()
    pl.semaphore_wait(barrier, total - 1)

    def sino_copy(source, block, target, send_sem):
        return pltpu.make_async_remote_copy(
            src_ref=source, dst_ref=all_sino.at[block], send_sem=send_sem,
            recv_sem=s_recv.at[block], device_id={"ang": target},
            device_id_type=pl.DeviceIdType.MESH,
        )

    for k in range(chips - 1, 0, -1):
        sino_copy(sino, me, lax.rem(chip + k, chips) * 2 + core, s_send.at[k]).start()
    sino_copy(sino, me, mate, f_send.at[0]).start()

    def coord_copy(j, t):
        place = lax.rem(me + j, share)
        side = lax.rem(half + t, halves)
        target = half * share + place
        return target, side, coords.at[place], c_send.at[j * halves + t]

    def coord_remote(j, t):
        target, side, block, sem = coord_copy(j, t)
        return pltpu.make_async_remote_copy(
            src_ref=block, dst_ref=all_coords.at[me], send_sem=sem,
            recv_sem=c_recv.at[me], device_id={"ang": target, "sl": side},
            device_id_type=pl.DeviceIdType.MESH,
        )

    source_half = me // share
    at_home = source_half == half
    for j in range(share):
        for t in range(halves):
            if j == 0 and t == 0:
                @pl.when(at_home)
                def _():
                    pltpu.make_async_copy(
                        coords.at[lax.rem(me, share)], all_coords.at[me], c_recv.at[me]
                    ).start()

                @pl.when(jnp.logical_not(at_home))
                def _():
                    coord_remote(0, 0).start()
            else:
                coord_remote(j, t).start()

    for k in range(1, chips):
        block = lax.rem(chip + k, chips) * 2 + core
        sino_copy(sino, block, mate, f_send.at[k]).wait_recv()
        sino_copy(all_sino.at[block], block, mate, f_send.at[k]).start()
    for k in range(chips):
        block = lax.rem(chip + k, chips) * 2 + 1 - core
        sino_copy(sino, block, mate, f_send.at[0]).wait_recv()
    for g in range(groups):
        pltpu.make_async_copy(coords.at[0], all_coords.at[g], c_recv.at[g]).wait()
    own.wait()
    for k in range(1, chips):
        sino_copy(sino, me, mate, s_send.at[k]).wait_send()
    for k in range(chips):
        sino_copy(sino, me, mate, f_send.at[k]).wait_send()
    for j in range(share):
        for t in range(halves):
            if j == 0 and t == 0:
                @pl.when(jnp.logical_not(at_home))
                def _():
                    coord_remote(0, 0).wait_send()
            else:
                coord_remote(j, t).wait_send()


def shards(sinogram, detector_coord):
    slices, own_angles, bins = sinogram.shape
    local_rows, width = detector_coord.shape[1:]
    groups, halves = lax.axis_size("ang"), lax.axis_size("sl")
    row_share = local_rows * halves // groups
    share = local_rows // row_share
    sino = sinogram.reshape(slices * own_angles, bins)
    coords = detector_coord.reshape(own_angles, share, row_share, width)
    coords = coords.transpose(1, 0, 2, 3).reshape(share, -1, LANES)
    vmem = pl.BlockSpec(memory_space=pltpu.VMEM)
    all_sino, all_coords = pl.pallas_call(
        functools.partial(exchange_kernel, groups, halves),
        out_shape=(
            jax.ShapeDtypeStruct((groups,) + sino.shape, sino.dtype),
            jax.ShapeDtypeStruct((groups,) + coords.shape[1:], coords.dtype),
        ),
        in_specs=[vmem] * 2,
        out_specs=(vmem, vmem),
        scratch_shapes=[
            pltpu.SemaphoreType.DMA((1,)),
            pltpu.SemaphoreType.DMA((groups // 2,)),
            pltpu.SemaphoreType.DMA((groups,)),
            pltpu.SemaphoreType.DMA((groups // 2,)),
            pltpu.SemaphoreType.DMA((groups,)),
            pltpu.SemaphoreType.DMA((groups,)),
        ],
        compiler_params=pltpu.CompilerParams(collective_id=0, has_side_effects=True),
    )(sino, coords)
    size = 256
    return pl.pallas_call(
        functools.partial(project_kernel, own_angles),
        out_shape=jax.ShapeDtypeStruct((row_share, slices, width), jnp.float32),
        in_specs=[vmem] * 2,
        out_specs=vmem,
        scratch_shapes=[
            pltpu.VMEM((2 * (bins // size) - 1, size, size), jnp.bfloat16),
            pltpu.VMEM((groups * slices * own_angles * bins // LANES, LANES), jnp.float32),
        ],
    )(all_sino.reshape(groups * slices * own_angles, bins), all_coords)


def solution(mesh):
    in_specs = (P("sl", "ang", None), P("ang", "sl", None))
    out_specs = P("ang", "sl", None)
    return jax.shard_map(shards, mesh=mesh, in_specs=in_specs, out_specs=out_specs, check_vma=False)
```

```python
import functools
import math

import jax
import jax.numpy as jnp
from jax import lax
from jax.experimental import pallas as pl
from jax.experimental.pallas import tpu as pltpu
from jax.sharding import PartitionSpec as P

LANES = 128
FRACTION_BITS = 20


def ramp_block(size, shift):
    first = lax.broadcasted_iota(jnp.int32, (size, size), 0)
    second = lax.broadcasted_iota(jnp.int32, (size, size), 1)
    offset = second - first + shift
    offset_sq = jnp.maximum((offset * offset).astype(jnp.float32), jnp.float32(1.0))
    values = jnp.where(
        offset == 0,
        jnp.float32(0.25),
        jnp.where(
            (offset & 1) != 0, jnp.float32(-1.0 / math.pi**2) / offset_sq, jnp.float32(0.0)
        ),
    )
    return values.astype(jnp.bfloat16)


def build_ramp(ramp, size, count):
    for step in range(2 * count - 1):
        ramp[step] = ramp_block(size, (step - count + 1) * size)


def filter_rows(sino, ramp, tiles, size, count):
    rows = sino.shape[0]
    per_row = sino.shape[1] // LANES
    for out_block in range(count):
        total = None
        for in_block in range(count):
            part = jnp.dot(
                sino[:, in_block * size : (in_block + 1) * size],
                ramp[out_block - in_block + count - 1],
                preferred_element_type=jnp.float32,
            )
            total = part if total is None else total + part
        total = total.astype(jnp.bfloat16).astype(jnp.float32)
        for piece in range(size // LANES):
            h = out_block * (size // LANES) + piece
            tiles[pl.ds(h, rows, stride=per_row), :] = total[:, piece * LANES : (piece + 1) * LANES]


def pick(tile, index):
    return jnp.take_along_axis(tile, index, axis=1, mode="promise_in_bounds")


def interpolate(coords, tiles, out, scale, own_angles, together=2):
    rows, slices, width = out.shape
    groups = coords.shape[0]
    per_row = tiles.shape[0] // (groups * slices * own_angles)
    across = width // LANES
    level = lax.broadcasted_iota(jnp.int32, (per_row, LANES), 0)
    spots = [(r, x) for r in range(rows) for x in range(across)]
    for start in range(0, len(spots), together):
        group = spots[start : start + together]

        def one_group(g, sums):
            sums = list(sums)
            for al in range(own_angles):
                picks = []
                for r, x in group:
                    c = coords[g, pl.ds((al * rows + r) * across + x, 1), :]
                    c = jnp.broadcast_to(c, (per_row, LANES))
                    left = c >> FRACTION_BITS
                    right = left + 1
                    fraction = (c & (2**FRACTION_BITS - 1)).astype(jnp.float32) * jnp.float32(
                        2.0**-FRACTION_BITS
                    )
                    w_left = (1.0 - fraction).astype(jnp.bfloat16).astype(jnp.float32)
                    w_right = fraction.astype(jnp.bfloat16).astype(jnp.float32)
                    w_left = jnp.where(left >> 7 == level, w_left, 0.0)
                    w_right = jnp.where(right >> 7 == level, w_right, 0.0)
                    picks.append((left & (LANES - 1), right & (LANES - 1), w_left, w_right))
                held = []
                for s in range(slices):
                    row = ((g * slices + s) * own_angles + al) * per_row
                    held.append(tiles[pl.ds(pl.multiple_of(row, per_row), per_row), :])
                for i, (i_left, i_right, w_left, w_right) in enumerate(picks):
                    for index, weight in ((i_left, w_left), (i_right, w_right)):
                        for s in range(slices):
                            at = s * len(group) + i
                            sums[at] = sums[at] + weight * pick(held[s], index)
            return tuple(sums)

        zero = jnp.zeros((per_row, LANES), jnp.float32)
        sums = lax.fori_loop(0, groups, one_group, (zero,) * (slices * len(group)))
        for s in range(slices):
            for i, (r, x) in enumerate(group):
                line = jnp.sum(sums[s * len(group) + i], axis=0, keepdims=True) * scale
                out[r, pl.ds(s, 1), pl.ds(x * LANES, LANES)] = line


def project_kernel(own_angles, sino, coords, out, ramp, tiles):
    bins = sino.shape[1]
    size = ramp.shape[1]
    build_ramp(ramp, size, bins // size)
    filter_rows(sino, ramp, tiles, size, bins // size)
    scale = jnp.float32(math.pi / (own_angles * coords.shape[0]))
    interpolate(coords, tiles, out, scale, own_angles)


def exchange_kernel(
    groups, halves, sino, coords, all_sino, all_coords,
    local_sem, s_send, n_send, f_send, s_recv, c_send, x_send, c_recv,
):
    me, half = lax.axis_index("ang"), lax.axis_index("sl")
    outer, outers = me // 4, groups // 4
    mate = me + 1 - 2 * (me % 2)
    near = me + 2 - 4 * (me // 2 % 2)
    total = groups * halves
    share = coords.shape[0]

    barrier = pltpu.get_barrier_semaphore()

    def greet(k, carry):
        there = lax.rem(me * halves + half + k, total)
        pl.semaphore_signal(
            barrier, inc=1, device_id={"ang": there // halves, "sl": there % halves},
            device_id_type=pl.DeviceIdType.MESH,
        )
        return carry

    lax.fori_loop(1, total, greet, 0)
    own = pltpu.make_async_copy(sino, all_sino.at[me], local_sem.at[0])
    own.start()
    pl.semaphore_wait(barrier, total - 1)

    def sino_copy(block, target, send_sem, source=None):
        return pltpu.make_async_remote_copy(
            src_ref=all_sino.at[block] if source is None else source,
            dst_ref=all_sino.at[block], send_sem=send_sem,
            recv_sem=s_recv.at[block], device_id={"ang": target},
            device_id_type=pl.DeviceIdType.MESH,
        )

    def coord_copy(block, target, side, send_sem, source=None):
        return pltpu.make_async_remote_copy(
            src_ref=all_coords.at[block] if source is None else source,
            dst_ref=all_coords.at[block], send_sem=send_sem,
            recv_sem=c_recv.at[block], device_id={"ang": target, "sl": side},
            device_id_type=pl.DeviceIdType.MESH,
        )

    def far(k):
        return lax.rem(outer + k, outers) * 4 + me % 4

    primary = me // share == half
    for k in range(1, outers):
        sino_copy(me, far(k), s_send.at[k], sino).start()
    sino_copy(me, near, n_send.at[0], sino).start()
    sino_copy(me, mate, f_send.at[0], sino).start()
    for j in range(1, share):
        place = lax.rem(me + j, share)
        coord_copy(me, half * share + place, half, c_send.at[j], coords.at[place]).start()
    home = lax.rem(me, share)

    @pl.when(primary)
    def _():
        pltpu.make_async_copy(coords.at[home], all_coords.at[me], c_recv.at[me]).start()

    @pl.when(jnp.logical_not(primary))
    def _():
        coord_copy(me, half * share + home, half, c_send.at[0], coords.at[home]).start()

    def arrived(block):
        sino_copy(block, mate, s_send.at[0]).wait_recv()

    for k in range(1, outers):
        arrived(far(k))
        sino_copy(far(k), near, n_send.at[k]).start()
        sino_copy(far(k), mate, f_send.at[k]).start()

    def spread(g):
        pltpu.make_async_copy(coords.at[0], all_coords.at[g], c_recv.at[g]).wait()

        @pl.when(primary)
        def _():
            for t in range(1, halves):
                side = lax.rem(half + t, halves)
                coord_copy(g, me, side, x_send.at[g * (halves - 1) + t - 1]).start()

    def from_near(k):
        return lax.rem(outer + k, outers) * 4 + near % 4

    for k in range(outers):
        for i in range(4):
            spread(lax.rem(outer + k, outers) * 4 + i)
        arrived(from_near(k))
        sino_copy(from_near(k), mate, f_send.at[outers + k]).start()
    for k in range(outers):
        arrived(lax.rem(outer + k, outers) * 4 + mate % 4)
        arrived(lax.rem(outer + k, outers) * 4 + 3 - me % 4)
    own.wait()
    for k in range(1, outers):
        sino_copy(me, mate, s_send.at[k]).wait_send()
    for k in range(outers):
        sino_copy(me, mate, n_send.at[k]).wait_send()
    for k in range(2 * outers):
        sino_copy(me, mate, f_send.at[k]).wait_send()
    for j in range(1, share):
        coord_copy(me, mate, half, c_send.at[j]).wait_send()

    @pl.when(jnp.logical_not(primary))
    def _():
        coord_copy(me, mate, half, c_send.at[0]).wait_send()

    @pl.when(primary)
    def _():
        for i in range(groups * (halves - 1)):
            coord_copy(me, mate, half, x_send.at[i]).wait_send()


def shards(sinogram, detector_coord):
    slices, own_angles, bins = sinogram.shape
    local_rows, width = detector_coord.shape[1:]
    groups, halves = lax.axis_size("ang"), lax.axis_size("sl")
    row_share = local_rows * halves // groups
    share = local_rows // row_share
    sino = sinogram.reshape(slices * own_angles, bins)
    coords = detector_coord.reshape(own_angles, share, row_share, width)
    coords = coords.transpose(1, 0, 2, 3).reshape(share, -1, LANES)
    vmem = pl.BlockSpec(memory_space=pltpu.VMEM)
    all_sino, all_coords = pl.pallas_call(
        functools.partial(exchange_kernel, groups, halves),
        out_shape=(
            jax.ShapeDtypeStruct((groups,) + sino.shape, sino.dtype),
            jax.ShapeDtypeStruct((groups,) + coords.shape[1:], coords.dtype),
        ),
        in_specs=[vmem] * 2,
        out_specs=(vmem, vmem),
        scratch_shapes=[
            pltpu.SemaphoreType.DMA((1,)),
            pltpu.SemaphoreType.DMA((groups // 4,)),
            pltpu.SemaphoreType.DMA((groups // 4,)),
            pltpu.SemaphoreType.DMA((groups // 2,)),
            pltpu.SemaphoreType.DMA((groups,)),
            pltpu.SemaphoreType.DMA((share,)),
            pltpu.SemaphoreType.DMA((groups * (halves - 1),)),
            pltpu.SemaphoreType.DMA((groups,)),
        ],
        compiler_params=pltpu.CompilerParams(collective_id=0, has_side_effects=True),
    )(sino, coords)
    size = 256
    return pl.pallas_call(
        functools.partial(project_kernel, own_angles),
        out_shape=jax.ShapeDtypeStruct((row_share, slices, width), jnp.float32),
        in_specs=[vmem] * 2,
        out_specs=vmem,
        scratch_shapes=[
            pltpu.VMEM((2 * (bins // size) - 1, size, size), jnp.bfloat16),
            pltpu.VMEM((groups * slices * own_angles * bins // LANES, LANES), jnp.float32),
        ],
    )(all_sino.reshape(groups * slices * own_angles, bins), all_coords)


def solution(mesh):
    in_specs = (P("sl", "ang", None), P("ang", "sl", None))
    out_specs = P("ang", "sl", None)
    return jax.shard_map(shards, mesh=mesh, in_specs=in_specs, out_specs=out_specs, check_vma=False)
```

```python
import functools
import math

import jax
import jax.numpy as jnp
from jax import lax
from jax.experimental import pallas as pl
from jax.experimental.pallas import tpu as pltpu
from jax.sharding import PartitionSpec as P

LANES = 128
FRACTION_BITS = 20


def ramp_block(size, shift):
    first = lax.broadcasted_iota(jnp.int32, (size, size), 0)
    second = lax.broadcasted_iota(jnp.int32, (size, size), 1)
    offset = second - first + shift
    offset_sq = jnp.maximum((offset * offset).astype(jnp.float32), jnp.float32(1.0))
    values = jnp.where(
        offset == 0,
        jnp.float32(0.25),
        jnp.where(
            (offset & 1) != 0, jnp.float32(-1.0 / math.pi**2) / offset_sq, jnp.float32(0.0)
        ),
    )
    return values.astype(jnp.bfloat16)


def build_ramp(ramp, size, count):
    for step in range(2 * count - 1):
        ramp[step] = ramp_block(size, (step - count + 1) * size)


def filter_rows(sino, ramp, tiles, size, count):
    rows = sino.shape[0] * sino.shape[1]
    per_row = sino.shape[2] // LANES
    for out_block in range(count):
        total = None
        for in_block in range(count):
            part = jnp.dot(
                sino[:, :, in_block * size : (in_block + 1) * size].reshape(rows, size),
                ramp[out_block - in_block + count - 1],
                preferred_element_type=jnp.float32,
            )
            total = part if total is None else total + part
        total = total.astype(jnp.bfloat16).astype(jnp.float32)
        for piece in range(size // LANES):
            h = out_block * (size // LANES) + piece
            tiles[pl.ds(h, rows, stride=per_row), :] = total[:, piece * LANES : (piece + 1) * LANES]


def pick(tile, index):
    return jnp.take_along_axis(tile, index, axis=1, mode="promise_in_bounds")


def interpolate(coords, tiles, out, scale, own_angles, together=2):
    rows, slices, width = out.shape
    groups = coords.shape[0]
    per_row = tiles.shape[0] // (groups * slices * own_angles)
    across = width // LANES
    level = lax.broadcasted_iota(jnp.int32, (per_row, LANES), 0)
    spots = [(r, x) for r in range(rows) for x in range(across)]
    for start in range(0, len(spots), together):
        group = spots[start : start + together]

        def one_group(g, sums):
            sums = list(sums)
            for al in range(own_angles):
                picks = []
                for r, x in group:
                    c = coords[g, pl.ds((al * rows + r) * across + x, 1), :]
                    c = jnp.broadcast_to(c, (per_row, LANES))
                    left = c >> FRACTION_BITS
                    right = left + 1
                    fraction = (c & (2**FRACTION_BITS - 1)).astype(jnp.float32) * jnp.float32(
                        2.0**-FRACTION_BITS
                    )
                    w_left = (1.0 - fraction).astype(jnp.bfloat16).astype(jnp.float32)
                    w_right = fraction.astype(jnp.bfloat16).astype(jnp.float32)
                    w_left = jnp.where(left >> 7 == level, w_left, 0.0)
                    w_right = jnp.where(right >> 7 == level, w_right, 0.0)
                    picks.append((left & (LANES - 1), right & (LANES - 1), w_left, w_right))
                held = []
                for s in range(slices):
                    row = ((g * slices + s) * own_angles + al) * per_row
                    held.append(tiles[pl.ds(pl.multiple_of(row, per_row), per_row), :])
                for i, (i_left, i_right, w_left, w_right) in enumerate(picks):
                    for index, weight in ((i_left, w_left), (i_right, w_right)):
                        for s in range(slices):
                            at = s * len(group) + i
                            sums[at] = sums[at] + weight * pick(held[s], index)
            return tuple(sums)

        zero = jnp.zeros((per_row, LANES), jnp.float32)
        sums = lax.fori_loop(0, groups, one_group, (zero,) * (slices * len(group)))
        for s in range(slices):
            for i, (r, x) in enumerate(group):
                line = jnp.sum(sums[s * len(group) + i], axis=0, keepdims=True) * scale
                out[r, pl.ds(s, 1), pl.ds(x * LANES, LANES)] = line


def kernel(
    groups, halves, own_angles, sino, coords, out, all_sino, all_coords, ramp, tiles,
    local_sem, s_send, n_send, f_send, s_recv, c_send, x_send, c_recv,
):
    me, half = lax.axis_index("ang"), lax.axis_index("sl")
    outer, outers = me // 4, groups // 4
    mate = me + 1 - 2 * (me % 2)
    near = me + 2 - 4 * (me // 2 % 2)
    total = groups * halves
    share = coords.shape[0]

    barrier = pltpu.get_barrier_semaphore()

    def greet(k, carry):
        there = lax.rem(me * halves + half + k, total)
        pl.semaphore_signal(
            barrier, inc=1, device_id={"ang": there // halves, "sl": there % halves},
            device_id_type=pl.DeviceIdType.MESH,
        )
        return carry

    lax.fori_loop(1, total, greet, 0)
    own = pltpu.make_async_copy(sino, all_sino.at[me], local_sem.at[0])
    own.start()
    bins, size = sino.shape[1], ramp.shape[1]
    build_ramp(ramp, size, bins // size)
    pl.semaphore_wait(barrier, total - 1)

    def sino_copy(block, target, send_sem, source=None):
        return pltpu.make_async_remote_copy(
            src_ref=all_sino.at[block] if source is None else source,
            dst_ref=all_sino.at[block], send_sem=send_sem,
            recv_sem=s_recv.at[block], device_id={"ang": target},
            device_id_type=pl.DeviceIdType.MESH,
        )

    def coord_copy(block, target, side, send_sem, source=None):
        return pltpu.make_async_remote_copy(
            src_ref=all_coords.at[block] if source is None else source,
            dst_ref=all_coords.at[block], send_sem=send_sem,
            recv_sem=c_recv.at[block], device_id={"ang": target, "sl": side},
            device_id_type=pl.DeviceIdType.MESH,
        )

    def far(k):
        return lax.rem(outer + k, outers) * 4 + me % 4

    primary = me // share == half
    for k in range(1, outers):
        sino_copy(me, far(k), s_send.at[k], sino).start()
    sino_copy(me, near, n_send.at[0], sino).start()
    sino_copy(me, mate, f_send.at[0], sino).start()
    for j in range(1, share):
        place = lax.rem(me + j, share)
        coord_copy(me, half * share + place, half, c_send.at[j], coords.at[place]).start()
    home = lax.rem(me, share)

    @pl.when(primary)
    def _():
        pltpu.make_async_copy(coords.at[home], all_coords.at[me], c_recv.at[me]).start()

    @pl.when(jnp.logical_not(primary))
    def _():
        coord_copy(me, half * share + home, half, c_send.at[0], coords.at[home]).start()

    def arrived(block):
        sino_copy(block, mate, s_send.at[0]).wait_recv()

    for k in range(1, outers):
        arrived(far(k))
        sino_copy(far(k), near, n_send.at[k]).start()
        sino_copy(far(k), mate, f_send.at[k]).start()

    def spread(g):
        pltpu.make_async_copy(coords.at[0], all_coords.at[g], c_recv.at[g]).wait()

        @pl.when(primary)
        def _():
            for t in range(1, halves):
                side = lax.rem(half + t, halves)
                coord_copy(g, me, side, x_send.at[g * (halves - 1) + t - 1]).start()

    def from_near(k):
        return lax.rem(outer + k, outers) * 4 + near % 4

    for k in range(outers):
        for i in range(4):
            spread(lax.rem(outer + k, outers) * 4 + i)
        arrived(from_near(k))
        sino_copy(from_near(k), mate, f_send.at[outers + k]).start()
    for k in range(outers):
        arrived(lax.rem(outer + k, outers) * 4 + mate % 4)
        arrived(lax.rem(outer + k, outers) * 4 + 3 - me % 4)
    own.wait()
    filter_rows(all_sino, ramp, tiles, size, bins // size)
    scale = jnp.float32(math.pi / (own_angles * groups))
    interpolate(all_coords, tiles, out, scale, own_angles)
    for k in range(1, outers):
        sino_copy(me, mate, s_send.at[k]).wait_send()
    for k in range(outers):
        sino_copy(me, mate, n_send.at[k]).wait_send()
    for k in range(2 * outers):
        sino_copy(me, mate, f_send.at[k]).wait_send()
    for j in range(1, share):
        coord_copy(me, mate, half, c_send.at[j]).wait_send()

    @pl.when(jnp.logical_not(primary))
    def _():
        coord_copy(me, mate, half, c_send.at[0]).wait_send()

    @pl.when(primary)
    def _():
        for i in range(groups * (halves - 1)):
            coord_copy(me, mate, half, x_send.at[i]).wait_send()


def shards(sinogram, detector_coord):
    slices, own_angles, bins = sinogram.shape
    local_rows, width = detector_coord.shape[1:]
    groups, halves = lax.axis_size("ang"), lax.axis_size("sl")
    row_share = local_rows * halves // groups
    share = local_rows // row_share
    sino = sinogram.reshape(slices * own_angles, bins)
    coords = detector_coord.reshape(own_angles, share, row_share, width)
    coords = coords.transpose(1, 0, 2, 3).reshape(share, -1, LANES)
    vmem = pl.BlockSpec(memory_space=pltpu.VMEM)
    size = 256
    return pl.pallas_call(
        functools.partial(kernel, groups, halves, own_angles),
        out_shape=jax.ShapeDtypeStruct((row_share, slices, width), jnp.float32),
        in_specs=[vmem] * 2,
        out_specs=vmem,
        scratch_shapes=[
            pltpu.VMEM((groups,) + sino.shape, sino.dtype),
            pltpu.VMEM((groups,) + coords.shape[1:], coords.dtype),
            pltpu.VMEM((2 * (bins // size) - 1, size, size), jnp.bfloat16),
            pltpu.VMEM((groups * slices * own_angles * bins // LANES, LANES), jnp.float32),
            pltpu.SemaphoreType.DMA((1,)),
            pltpu.SemaphoreType.DMA((groups // 4,)),
            pltpu.SemaphoreType.DMA((groups // 4,)),
            pltpu.SemaphoreType.DMA((groups // 2,)),
            pltpu.SemaphoreType.DMA((groups,)),
            pltpu.SemaphoreType.DMA((share,)),
            pltpu.SemaphoreType.DMA((groups * (halves - 1),)),
            pltpu.SemaphoreType.DMA((groups,)),
        ],
        compiler_params=pltpu.CompilerParams(collective_id=0, has_side_effects=True),
    )(sino, coords)


def solution(mesh):
    in_specs = (P("sl", "ang", None), P("ang", "sl", None))
    out_specs = P("ang", "sl", None)
    return jax.shard_map(shards, mesh=mesh, in_specs=in_specs, out_specs=out_specs, check_vma=False)
```

```python
import functools
import math

import jax
import jax.numpy as jnp
from jax import lax
from jax.experimental import pallas as pl
from jax.experimental.pallas import tpu as pltpu
from jax.sharding import PartitionSpec as P

LANES = 128
FRACTION_BITS = 20


def ramp_block(size, shift):
    first = lax.broadcasted_iota(jnp.int32, (size, size), 0)
    second = lax.broadcasted_iota(jnp.int32, (size, size), 1)
    offset = second - first + shift
    offset_sq = jnp.maximum((offset * offset).astype(jnp.float32), jnp.float32(1.0))
    values = jnp.where(
        offset == 0,
        jnp.float32(0.25),
        jnp.where(
            (offset & 1) != 0, jnp.float32(-1.0 / math.pi**2) / offset_sq, jnp.float32(0.0)
        ),
    )
    return values.astype(jnp.bfloat16)


def build_ramp(ramp, size, count):
    for step in range(2 * count - 1):
        ramp[step] = ramp_block(size, (step - count + 1) * size)


def filter_rows(sino, ramp, tiles, size, count):
    rows = sino.shape[0] * sino.shape[1]
    per_row = sino.shape[2] // LANES
    for out_block in range(count):
        total = None
        for in_block in range(count):
            part = jnp.dot(
                sino[:, :, in_block * size : (in_block + 1) * size].reshape(rows, size),
                ramp[out_block - in_block + count - 1],
                preferred_element_type=jnp.float32,
            )
            total = part if total is None else total + part
        total = total.astype(jnp.bfloat16).astype(jnp.float32)
        for piece in range(size // LANES):
            h = out_block * (size // LANES) + piece
            tiles[pl.ds(h, rows, stride=per_row), :] = total[:, piece * LANES : (piece + 1) * LANES]


def pick(tile, index):
    return jnp.take_along_axis(tile, index, axis=1, mode="promise_in_bounds")


def interpolate(coords, tiles, out, scale, own_angles, together=2):
    rows, slices, width = out.shape
    groups = coords.shape[0]
    per_row = tiles.shape[0] // (groups * slices * own_angles)
    across = width // LANES
    level = lax.broadcasted_iota(jnp.int32, (per_row, LANES), 0)
    spots = [(r, x) for r in range(rows) for x in range(across)]
    for start in range(0, len(spots), together):
        group = spots[start : start + together]

        def one_group(g, sums):
            sums = list(sums)
            for al in range(own_angles):
                picks = []
                for r, x in group:
                    c = coords[g, pl.ds((al * rows + r) * across + x, 1), :]
                    c = jnp.broadcast_to(c, (per_row, LANES))
                    left = c >> FRACTION_BITS
                    right = left + 1
                    fraction = (c & (2**FRACTION_BITS - 1)).astype(jnp.float32) * jnp.float32(
                        2.0**-FRACTION_BITS
                    )
                    w_left = (1.0 - fraction).astype(jnp.bfloat16).astype(jnp.float32)
                    w_right = fraction.astype(jnp.bfloat16).astype(jnp.float32)
                    w_left = jnp.where(left >> 7 == level, w_left, 0.0)
                    w_right = jnp.where(right >> 7 == level, w_right, 0.0)
                    picks.append((left & (LANES - 1), right & (LANES - 1), w_left, w_right))
                held = []
                for s in range(slices):
                    row = ((g * slices + s) * own_angles + al) * per_row
                    held.append(tiles[pl.ds(pl.multiple_of(row, per_row), per_row), :])
                for i, (i_left, i_right, w_left, w_right) in enumerate(picks):
                    for index, weight in ((i_left, w_left), (i_right, w_right)):
                        for s in range(slices):
                            at = s * len(group) + i
                            sums[at] = sums[at] + weight * pick(held[s], index)
            return tuple(sums)

        zero = jnp.zeros((per_row, LANES), jnp.float32)
        sums = lax.fori_loop(0, groups, one_group, (zero,) * (slices * len(group)))
        for s in range(slices):
            for i, (r, x) in enumerate(group):
                line = jnp.sum(sums[s * len(group) + i], axis=0, keepdims=True) * scale
                out[r, pl.ds(s, 1), pl.ds(x * LANES, LANES)] = line


def kernel(
    groups, halves, own_angles, sino, coords, out, all_sino, all_coords, ramp, tiles,
    local_sem, s_send, n_send, f_send, s_recv, c_send, x_send, c_recv,
):
    me, half = lax.axis_index("ang"), lax.axis_index("sl")
    outer, outers = me // 4, groups // 4
    mate = me + 1 - 2 * (me % 2)
    near = me + 2 - 4 * (me // 2 % 2)
    total = groups * halves
    share = coords.shape[0]

    barrier = pltpu.get_barrier_semaphore()

    def greet(k, carry):
        there = lax.rem(me * halves + half + k, total)
        pl.semaphore_signal(
            barrier, inc=1, device_id={"ang": there // halves, "sl": there % halves},
            device_id_type=pl.DeviceIdType.MESH,
        )
        return carry

    lax.fori_loop(1, total, greet, 0)
    own = pltpu.make_async_copy(sino, all_sino.at[me], local_sem.at[0])
    own.start()
    bins, size = sino.shape[1], ramp.shape[1]
    build_ramp(ramp, size, bins // size)
    pl.semaphore_wait(barrier, total - 1)

    def sino_copy(block, target, send_sem, source=None):
        return pltpu.make_async_remote_copy(
            src_ref=all_sino.at[block] if source is None else source,
            dst_ref=all_sino.at[block], send_sem=send_sem,
            recv_sem=s_recv.at[block], device_id={"ang": target},
            device_id_type=pl.DeviceIdType.MESH,
        )

    def coord_copy(block, target, side, send_sem, source=None):
        return pltpu.make_async_remote_copy(
            src_ref=all_coords.at[block] if source is None else source,
            dst_ref=all_coords.at[block], send_sem=send_sem,
            recv_sem=c_recv.at[block], device_id={"ang": target, "sl": side},
            device_id_type=pl.DeviceIdType.MESH,
        )

    def far(k):
        return lax.rem(outer + k, outers) * 4 + me % 4

    primary = me // share == half
    for k in range(1, outers):
        sino_copy(me, far(k), s_send.at[k], sino).start()
    sino_copy(me, near, n_send.at[0], sino).start()
    sino_copy(me, mate, f_send.at[0], sino).start()
    for j in range(1, share):
        place = lax.rem(me + j, share)
        coord_copy(me, half * share + place, half, c_send.at[j], coords.at[place]).start()
    home = lax.rem(me, share)

    @pl.when(primary)
    def _():
        pltpu.make_async_copy(coords.at[home], all_coords.at[me], c_recv.at[me]).start()

    @pl.when(jnp.logical_not(primary))
    def _():
        coord_copy(me, half * share + home, half, c_send.at[0], coords.at[home]).start()

    def arrived(block):
        sino_copy(block, mate, s_send.at[0]).wait_recv()

    for k in range(1, outers):
        arrived(far(k))
        sino_copy(far(k), near, n_send.at[k]).start()
        sino_copy(far(k), mate, f_send.at[k]).start()

    def coords_arrived(g):
        pltpu.make_async_copy(coords.at[0], all_coords.at[g], c_recv.at[g]).wait()

    def spread(g):
        coords_arrived(g)
        for t in range(1, halves):
            side = lax.rem(half + t, halves)
            coord_copy(g, me, side, x_send.at[g * (halves - 1) + t - 1]).start()

    def from_near(k):
        return lax.rem(outer + k, outers) * 4 + near % 4

    for k in range(outers):
        arrived(from_near(k))
        sino_copy(from_near(k), mate, f_send.at[outers + k]).start()

    @pl.when(primary)
    def _():
        for k in range(outers):
            for i in range(4):
                spread(lax.rem(outer + k, outers) * 4 + i)

    for k in range(outers):
        arrived(lax.rem(outer + k, outers) * 4 + mate % 4)
        arrived(lax.rem(outer + k, outers) * 4 + 3 - me % 4)
    own.wait()
    filter_rows(all_sino, ramp, tiles, size, bins // size)

    @pl.when(jnp.logical_not(primary))
    def _():
        for g in range(groups):
            coords_arrived(g)

    scale = jnp.float32(math.pi / (own_angles * groups))
    interpolate(all_coords, tiles, out, scale, own_angles)
    for k in range(1, outers):
        sino_copy(me, mate, s_send.at[k]).wait_send()
    for k in range(outers):
        sino_copy(me, mate, n_send.at[k]).wait_send()
    for k in range(2 * outers):
        sino_copy(me, mate, f_send.at[k]).wait_send()
    for j in range(1, share):
        coord_copy(me, mate, half, c_send.at[j]).wait_send()

    @pl.when(jnp.logical_not(primary))
    def _():
        coord_copy(me, mate, half, c_send.at[0]).wait_send()

    @pl.when(primary)
    def _():
        for i in range(groups * (halves - 1)):
            coord_copy(me, mate, half, x_send.at[i]).wait_send()


def shards(sinogram, detector_coord):
    slices, own_angles, bins = sinogram.shape
    local_rows, width = detector_coord.shape[1:]
    groups, halves = lax.axis_size("ang"), lax.axis_size("sl")
    row_share = local_rows * halves // groups
    share = local_rows // row_share
    sino = sinogram.reshape(slices * own_angles, bins)
    coords = detector_coord.reshape(own_angles, share, row_share, width)
    coords = coords.transpose(1, 0, 2, 3).reshape(share, -1, LANES)
    vmem = pl.BlockSpec(memory_space=pltpu.VMEM)
    size = 256
    return pl.pallas_call(
        functools.partial(kernel, groups, halves, own_angles),
        out_shape=jax.ShapeDtypeStruct((row_share, slices, width), jnp.float32),
        in_specs=[vmem] * 2,
        out_specs=vmem,
        scratch_shapes=[
            pltpu.VMEM((groups,) + sino.shape, sino.dtype),
            pltpu.VMEM((groups,) + coords.shape[1:], coords.dtype),
            pltpu.VMEM((2 * (bins // size) - 1, size, size), jnp.bfloat16),
            pltpu.VMEM((groups * slices * own_angles * bins // LANES, LANES), jnp.float32),
            pltpu.SemaphoreType.DMA((1,)),
            pltpu.SemaphoreType.DMA((groups // 4,)),
            pltpu.SemaphoreType.DMA((groups // 4,)),
            pltpu.SemaphoreType.DMA((groups // 2,)),
            pltpu.SemaphoreType.DMA((groups,)),
            pltpu.SemaphoreType.DMA((share,)),
            pltpu.SemaphoreType.DMA((groups * (halves - 1),)),
            pltpu.SemaphoreType.DMA((groups,)),
        ],
        compiler_params=pltpu.CompilerParams(collective_id=0, has_side_effects=True),
    )(sino, coords)


def solution(mesh):
    in_specs = (P("sl", "ang", None), P("ang", "sl", None))
    out_specs = P("ang", "sl", None)
    return jax.shard_map(shards, mesh=mesh, in_specs=in_specs, out_specs=out_specs, check_vma=False)
```
